32 devices in a mesh: dp: 8 (over z, y), mp: 4 (over x, core).
Axes of the slice: x: 2, y: 2, z: 4, core: 2. Of those that a mesh axis runs over, the one named last changes fastest.
Arguments:
- tokens: bfloat16 [49152, 512], P('dp'), may hold values from -6 to 6
- w_uvqk: bfloat16 [512, 2048], P(None, 'mp')
- w_out: bfloat16 [512, 512], replicated, may hold values from -0.25 to 0.25
- hist_len: int32 [8, 24], P('dp'), may hold values from 64 to 256, as said below
- owner: int32 [8, 24], P('dp'), may hold values from 0 to 7, as said below
- recv_offset: int32 [8, 24], P('dp'), may hold values from 0 to 47, as said below
- block_start: int32 [8, 24], P('dp'), may hold values from 0 to 47, as said below
Outputs:
- packed_out: bfloat16 [49152, 512], P('dp', 'mp')
- user_state: bfloat16 [192, 512], P('dp', 'mp')
The draws below stay inside these ranges and needn't reach their ends.
Inputs may be any that keep to these rules, and one draw needn't show every extreme that they name: User (d, u) has ceil(hist_len / 128) blocks, at most 2. owner[d, u] = (p(d) + r(u mod 8)) mod 8 for two permutations p, r of the indices of dp drawn from the seed: every owner receives exactly 24 users, and one device sends at most 3 users to one owner. On some owner every received user has 2 blocks. `recv_offset`: the users of one owner occupy disjoint runs of its 48 blocks, in the order of u; on some owner they fill all 48 blocks. `block_start`: the users of one device occupy disjoint runs of its 48 blocks, in the order of u.
All inputs are finite; a program needn't handle non-finite values.
Results may differ from the reference program's by a relative error of at most 0.0059.
Values may be sent and summed in bfloat16 or wider, within the bound.
A program may use at most 128 MiB of HBM per device.

```python
import jax
import jax.numpy as jnp
from jax import lax

D = 512
HEADS = 4
BLOCK = 128
MAXB = 2
USERS_DEV = 24
BLK_DEV = 48
ROWS = 49152
N_DP = 8


def place_runs(key, run_sizes, salt_value):
    before = jnp.cumsum(run_sizes, axis=1) - run_sizes
    spare_blocks = BLK_DEV - jnp.sum(run_sizes, axis=1, keepdims=True)
    gap_sums = jnp.cumsum(jax.random.randint(jax.random.fold_in(key, salt_value), run_sizes.shape, 0, 2), axis=1)
    return (before + jnp.minimum(gap_sums, spare_blocks)).astype(jnp.int32)


def draw_tables(key):
    device_count = N_DP
    user_count = USERS_DEV
    dev_perm = jax.random.permutation(jax.random.fold_in(key, 101), device_count).astype(jnp.int32)
    user_perm = jax.random.permutation(jax.random.fold_in(key, 102), device_count).astype(jnp.int32)
    user_ids = jnp.arange(user_count, dtype=jnp.int32)
    shifts = user_perm[user_ids % device_count]
    owners = ((dev_perm[:, None] + shifts[None, :]) % device_count).astype(jnp.int32)
    hottest = jax.random.randint(jax.random.fold_in(key, 103), (), 0, device_count)
    coin_flip = jax.random.randint(jax.random.fold_in(key, 104), (device_count, user_count), 0, 4)
    small_count = jax.random.randint(jax.random.fold_in(key, 108), (device_count, user_count), 1, MAXB + 1)
    counts = jnp.where(coin_flip > 0, MAXB, small_count)
    counts = jnp.where(owners == hottest, MAXB, counts).astype(jnp.int32)
    least_tail = jnp.where(counts == 1, BLOCK // 2, 1)
    extra_rows = jax.random.randint(jax.random.fold_in(key, 105), (device_count, user_count), 0, BLOCK + 1)
    last_fill = least_tail + extra_rows % (BLOCK + 1 - least_tail)
    lengths = ((counts - 1) * BLOCK + last_fill).astype(jnp.int32)
    starts = place_runs(key, counts, 106)
    inverse = jnp.zeros((device_count,), jnp.int32).at[dev_perm].set(jnp.arange(device_count, dtype=jnp.int32))
    sources = inverse[(jnp.arange(device_count, dtype=jnp.int32)[:, None] - shifts[None, :]) % device_count]
    incoming = counts[sources, user_ids[None, :]]
    landing = place_runs(key, incoming, 107)
    offsets = landing[owners, user_ids[None, :]].astype(jnp.int32)
    return (lengths, owners, offsets, starts)


def draw_hist_len(key, part):
    return draw_tables(key)[0]


def draw_owner(key, part):
    return draw_tables(key)[1]


def draw_recv_offset(key, part):
    return draw_tables(key)[2]


def draw_block_start(key, part):
    return draw_tables(key)[3]


def draw_w_uvqk(key, part):
    base_draw = jax.random.normal(jax.random.fold_in(key, 1), (D, 4 * D), jnp.float32)
    log_scale = jax.random.uniform(jax.random.fold_in(key, 2), (1, 4 * D), jnp.float32, -1.2, 1.2)
    return (base_draw * jnp.exp(log_scale) / jnp.sqrt(D * 1.0)).astype(jnp.bfloat16)


def shard_levels(rng, extent, split, least, high):
    factor_of = 1.0
    for dim, parts in split:
        steps = jax.random.uniform(jax.random.fold_in(jax.random.fold_in(rng, 6), dim), (parts,), jnp.float32, least / len(split), high / len(split))
        factor_of = factor_of * jnp.repeat(jnp.exp(steps), extent[dim] // parts).reshape((-1,) + (1,) * (len(extent) - 1 - dim))
    return factor_of


def normal_values(key, extent, spread, bound, split=(), held_as=jnp.bfloat16):
    values = jax.random.normal(key, extent, jnp.float32) * spread
    if len(split) > 0:
        values = shard_levels(key, extent, split, -0.22, 0.18) * values
    return jnp.clip(values, min=-bound, max=bound).astype(held_as)


def setup_inputs(seed: int = 0) -> dict:
    key_of = jax.random.split(jax.random.key(seed), 8)
    tokens = normal_values(key_of[0], (ROWS, D), 1.0, 6.0, ((0, 8),))
    w_uvqk = draw_w_uvqk(jax.random.fold_in(key_of[7], 71), 0)
    w_out = normal_values(key_of[2], (D, D), D ** -0.5, 0.25)
    hist_len = draw_hist_len(jax.random.fold_in(key_of[7], 71), 0)
    owner = draw_owner(jax.random.fold_in(key_of[7], 71), 0)
    recv_offset = draw_recv_offset(jax.random.fold_in(key_of[7], 71), 0)
    block_start = draw_block_start(jax.random.fold_in(key_of[7], 71), 0)
    return dict(tokens=tokens, w_uvqk=w_uvqk, w_out=w_out, hist_len=hist_len, owner=owner, recv_offset=recv_offset, block_start=block_start)


EPS = 1e-05

def norm_rows(values):
    average = lax.optimization_barrier(jnp.mean(values, axis=-1, keepdims=True))
    variance = lax.optimization_barrier(jnp.mean(values * values, axis=-1, keepdims=True)) - average * average
    return (values - average) * lax.rsqrt(variance + EPS)

def rounded(values):
    return lax.optimization_barrier(values.astype(jnp.bfloat16)).astype(jnp.float32)

def reference(tokens, w_uvqk, w_out, hist_len, owner, recv_offset, block_start):
    head_size = D // HEADS
    window_rows = MAXB * BLOCK
    total_rows = tokens.shape[0]
    device_count = hist_len.shape[0]
    user_count = hist_len.shape[1]
    padded = jnp.concatenate([tokens, jnp.zeros((window_rows, D), tokens.dtype)], 0)
    position = jnp.arange(window_rows, dtype=jnp.int32)
    causal = position[None, :] <= position[:, None]
    device_ids = (jnp.arange(device_count * user_count, dtype=jnp.int32) // user_count).astype(jnp.int32)
    flat_len = hist_len.reshape(-1).astype(jnp.int32)
    flat_start = block_start.reshape(-1).astype(jnp.int32)
    flat_owner = owner.reshape(-1).astype(jnp.int32)
    flat_offset = recv_offset.reshape(-1).astype(jnp.int32)

    def one_user(user_item):
        device_id, length, start = user_item
        first_row = ((device_id * BLK_DEV + start) * BLOCK).astype(jnp.int32)
        rows_in = lax.dynamic_slice_in_dim(padded, first_row, window_rows, 0)
        widened = rows_in.astype(jnp.float32)
        normed = norm_rows(widened).astype(jnp.bfloat16)
        projected = jax.nn.silu(jnp.dot(normed, w_uvqk, preferred_element_type=jnp.float32))
        pieces = rounded(projected).reshape(window_rows, HEADS, 4, head_size)
        raw_scores = jnp.einsum('ihd,jhd->hij', pieces[:, :, 2], pieces[:, :, 3]) * head_size ** (-0.5)
        allowed = causal & (position[None, :] < length)
        weights = rounded(jnp.where(allowed[None], jax.nn.silu(raw_scores) / window_rows, 0.0))
        attended = jnp.einsum('hij,jhd->ihd', weights, pieces[:, :, 1]).reshape(window_rows, D)
        gated_rows = (norm_rows(attended) * pieces[:, :, 0].reshape(window_rows, D)).astype(jnp.bfloat16)
        mixed_rows = jnp.dot(gated_rows, w_out, preferred_element_type=jnp.float32) + widened
        return mixed_rows.astype(jnp.bfloat16)
    outputs = lax.map(one_user, (device_ids, flat_len, flat_start))
    targets = ((flat_owner * BLK_DEV + flat_offset) * BLOCK)[:, None] + position[None, :]
    targets = jnp.where(position[None, :] < flat_len[:, None], targets, total_rows).astype(jnp.int32)
    packed = jnp.zeros((total_rows + 1, D), jnp.bfloat16)
    packed = packed.at[targets.reshape(-1)].set(outputs.reshape(-1, D))[:total_rows]
    user_state = outputs[jnp.arange(device_count * user_count, dtype=jnp.int32), flat_len - 1]
    return (packed, user_state)
```

```python
import functools

import jax
import jax.numpy as jnp
from jax import lax
from jax.experimental import pallas as pl
from jax.experimental.pallas import tpu as pltpu
from jax.sharding import PartitionSpec as P

D = 512
HEADS = 4
HEAD = D // HEADS
BLOCK = 128
MAXB = 2
WIN = MAXB * BLOCK
EPS = 1e-05
MESH = pl.DeviceIdType.MESH


def norm_rows(values):
    average = jnp.mean(values, axis=-1, keepdims=True)
    variance = jnp.mean(values * values, axis=-1, keepdims=True) - average * average
    return (values - average) * lax.rsqrt(variance + EPS)


def layer_kernel(
    dp_size, mp_size, per_pair,
    table, tok_hbm, w_ref, wout_ref, meta_ref,
    arr, meta_in, state_in,
    tok, wg, wop, normed, att, gate, send, state_out,
    tok_sem, own_sem, w_send, w_recv, meta_send, meta_recv, send_sem, recv_sem,
    state_send, state_recv,
):
    d = lax.axis_index("dp")
    m = lax.axis_index("mp")
    blocks = tok_hbm.shape[0]
    quarter = D // mp_size
    reach = dp_size // mp_size
    slots = reach * per_pair

    tok_copy = pltpu.make_async_copy(tok_hbm, tok.at[pl.ds(0, blocks)], tok_sem)
    tok_copy.start()
    own_copy = pltpu.make_async_copy(w_ref, wg.at[0], own_sem)
    own_copy.start()

    barrier = pltpu.get_barrier_semaphore()

    def greet(step, carry):
        o = lax.rem(d + step // mp_size, dp_size)
        q = lax.rem(m + lax.rem(step, mp_size), mp_size)
        pl.semaphore_signal(barrier, inc=1, device_id={"dp": o, "mp": q}, device_id_type=MESH)
        return carry

    lax.fori_loop(1, dp_size * mp_size, greet, 0)
    pl.semaphore_wait(barrier, dp_size * mp_size - 1)

    def flip(bits):
        if bits == 1:
            return m + 1 - 2 * lax.rem(m, 2)
        return lax.rem(m + 2, 4)

    def w_copy(src, slot, peer, index):
        return pltpu.make_async_remote_copy(
            src_ref=src, dst_ref=wg.at[slot], send_sem=w_send.at[index],
            recv_sem=w_recv.at[index], device_id={"mp": peer}, device_id_type=MESH,
        )

    far = w_copy(w_ref, 2, flip(2), 1)
    far.start()
    near = w_copy(w_ref, 1, flip(1), 0)
    near.start()
    relay = w_copy(wg.at[2], 3, flip(1), 2)

    def meta_copy(step):
        o = lax.rem(d + step, dp_size)
        return pltpu.make_async_remote_copy(
            src_ref=meta_ref.at[o], dst_ref=meta_in.at[d], send_sem=meta_send.at[step],
            recv_sem=meta_recv.at[d], device_id={"dp": o}, device_id_type=MESH,
        )

    def start_meta(step, carry):
        meta_copy(step).start()
        return carry

    lax.fori_loop(1, dp_size, start_meta, 0)
    meta_local = pltpu.make_async_copy(meta_ref.at[d], meta_in.at[d], meta_recv.at[d])
    meta_local.start()

    tok[blocks] = jnp.zeros((BLOCK, D), jnp.bfloat16)
    for bits in range(mp_size):
        head = m
        if bits & 1:
            head = head + 1 - 2 * lax.rem(head, 2)
        if bits & 2:
            head = lax.rem(head + 2, 4)
        wop[bits * HEAD : (bits + 1) * HEAD, :] = wout_ref[
            pl.ds(pl.multiple_of(head * HEAD, HEAD), HEAD), :
        ]
    tok_copy.wait()

    def target(s):
        k = s // per_pair
        j = s - k * per_pair
        return lax.rem(d + m + mp_size * (reach - 1 - k), dp_size), j

    def rows_of(s):
        o, j = target(s)
        start = table[o, 4 * j]
        return jnp.concatenate([tok[start], tok[start + 1]], 0)

    causal = lax.broadcasted_iota(jnp.int32, (BLOCK, BLOCK), 1) <= lax.broadcasted_iota(
        jnp.int32, (BLOCK, BLOCK), 0
    )
    half_scale = 0.5 * HEAD ** (-0.5)

    def scores(q, k):
        t = lax.dot_general(
            q, k, (((1,), (1,)), ((), ())), preferred_element_type=jnp.float32
        ) * half_scale
        return t + t * jnp.tanh(t)

    def one_head(rows_in, bits):
        h = jnp.dot(rows_in, wg[bits], preferred_element_type=jnp.float32) * 0.5
        p = (h + h * jnp.tanh(h)).astype(jnp.bfloat16)
        u, v, q, k = (p[:, i * HEAD : (i + 1) * HEAD] for i in range(4))
        low = jnp.where(causal, scores(q[:BLOCK], k[:BLOCK]), 0.0).astype(jnp.bfloat16)
        back = scores(q[BLOCK:], k[:BLOCK])
        diag = jnp.where(causal, scores(q[BLOCK:], k[BLOCK:]), 0.0)
        high = jnp.concatenate([back, diag], 1).astype(jnp.bfloat16)
        first = jnp.dot(low, v[:BLOCK], preferred_element_type=jnp.float32)
        second = jnp.dot(high, v, preferred_element_type=jnp.float32)
        return u, jnp.concatenate([first, second], 0) * (1.0 / WIN)

    own_copy.wait()
    near.wait()

    def early(s, carry):
        n = norm_rows(rows_of(s).astype(jnp.float32)).astype(jnp.bfloat16)
        normed[s] = n
        for bits in (0, 1):
            u, a = one_head(n, bits)
            gate[s, bits] = u
            att[s, bits] = a
        return carry

    lax.fori_loop(0, slots, early, 0)

    far.wait()
    relay.start()
    relay.wait()

    def send_copy(s, q):
        o, j = target(s)
        return pltpu.make_async_remote_copy(
            src_ref=send.at[s, q], dst_ref=arr.at[d * per_pair + j],
            send_sem=send_sem.at[s, q], recv_sem=recv_sem.at[d * per_pair + j],
            device_id={"dp": o, "mp": q}, device_id_type=MESH,
        )

    def each_target(s, remote):
        o, j = target(s)
        for q in range(mp_size):
            own = jnp.logical_and(o == d, m == q)

            @pl.when(jnp.logical_not(own))
            def _():
                remote(s, q)

            if remote is start_send:

                @pl.when(own)
                def _():
                    pltpu.make_async_copy(
                        send.at[s, q], arr.at[d * per_pair + j], recv_sem.at[d * per_pair + j]
                    ).start()

    def start_send(s, q):
        send_copy(s, q).start()

    def end_send(s, q):
        send_copy(s, q).wait_send()

    picks = lax.broadcasted_iota(jnp.int32, (8, WIN), 1)

    def late(s, carry):
        n = normed[s]
        parts = [(gate[s, 0], att[s, 0]), (gate[s, 1], att[s, 1])]
        parts += [one_head(n, 2), one_head(n, 3)]
        a = jnp.concatenate([part[1] for part in parts], 1)
        g = jnp.concatenate([part[0] for part in parts], 1).astype(jnp.float32)
        gated = (norm_rows(a) * g).astype(jnp.bfloat16)
        y = jnp.dot(gated, wop[...], preferred_element_type=jnp.float32)
        y = (y + rows_of(s).astype(jnp.float32)).astype(jnp.bfloat16)
        o, j = target(s)
        last = table[o, 4 * j + 1] - 1
        pick = (picks == last).astype(jnp.bfloat16)
        chosen = jnp.dot(pick, y, preferred_element_type=jnp.float32)
        for q in range(mp_size):
            send[s, q] = y[:, q * quarter : (q + 1) * quarter]
            state_out[q, pl.ds(s, 1), :] = chosen[0:1, q * quarter : (q + 1) * quarter]
        each_target(s, start_send)
        return carry

    lax.fori_loop(0, slots, late, 0)

    def state_copy(step):
        q = lax.rem(m + step, mp_size)
        return pltpu.make_async_remote_copy(
            src_ref=state_out.at[q], dst_ref=state_in.at[m], send_sem=state_send.at[step],
            recv_sem=state_recv.at[m], device_id={"mp": q}, device_id_type=MESH,
        )

    for step in range(1, mp_size):
        state_copy(step).start()
    state_local = pltpu.make_async_copy(state_out.at[m], state_in.at[m], state_recv.at[m])
    state_local.start()

    def end_meta(step, carry):
        meta_copy(step).wait_send()
        return carry

    lax.fori_loop(1, dp_size, end_meta, 0)

    def got_meta(src, carry):
        pltpu.make_async_copy(meta_ref.at[src], meta_in.at[src], meta_recv.at[src]).wait()
        return carry

    lax.fori_loop(0, dp_size, got_meta, 0)

    def sent(s, carry):
        each_target(s, end_send)
        return carry

    lax.fori_loop(0, slots, sent, 0)

    def got(i, carry):
        pltpu.make_async_copy(send.at[0, 0], arr.at[i], recv_sem.at[i]).wait()
        return carry

    lax.fori_loop(0, dp_size * per_pair, got, 0)
    for step in range(1, mp_size):
        state_copy(step).wait_send()
    for q in range(mp_size):
        pltpu.make_async_copy(state_out.at[q], state_in.at[q], state_recv.at[q]).wait()


def place_kernel(dp_size, per_pair, meta, user_pos, arr, state_in, packed, state, rows32):
    slots = state_in.shape[1]
    packed[...] = jnp.zeros(packed.shape, packed.dtype)
    row = lax.broadcasted_iota(jnp.int32, (BLOCK, packed.shape[1]), 0)

    def one(i, carry):
        src = i // per_pair
        j = i - src * per_pair
        length = meta[src, 0, 4 * j + 1]
        offset = meta[src, 0, 4 * j + 2]
        for b in range(MAXB):
            fill = length - b * BLOCK

            @pl.when(fill > 0)
            def _():
                value = arr[i, b * BLOCK : (b + 1) * BLOCK, :].astype(jnp.float32)
                value = jnp.where(row < fill, value, 0.0).astype(packed.dtype)
                packed[pl.ds(pl.multiple_of((offset + b) * BLOCK, BLOCK), BLOCK), :] = value

        return carry

    lax.fori_loop(0, dp_size * per_pair, one, 0)

    def pick(u, carry):
        pos = user_pos[u]
        q = pos // slots
        rows32[pl.ds(u, 1), :] = state_in[q, pl.ds(pos - q * slots, 1), :]
        return carry

    lax.fori_loop(0, state.shape[0], pick, 0)
    state[...] = rows32[...].astype(state.dtype)


def per_device(tokens, w_uvqk, w_out, hist_len, owner, recv_offset, block_start):
    dp_size = lax.axis_size("dp")
    mp_size = lax.axis_size("mp")
    d = lax.axis_index("dp")
    user_count = hist_len.shape[1]
    per_pair = -(-user_count // dp_size)
    pairs = dp_size * per_pair
    slots = (dp_size // mp_size) * per_pair
    slots_pad = -(-slots // 8) * 8
    quarter = D // mp_size
    rows = tokens.shape[0]
    lengths, owners, offsets, starts = hist_len[0], owner[0], recv_offset[0], block_start[0]
    ids = jnp.arange(user_count, dtype=jnp.int32)
    earlier = (owners[:, None] == owners[None, :]) & (ids[None, :] < ids[:, None])
    rank = jnp.sum(earlier.astype(jnp.int32), axis=1)
    lane = jnp.arange(128, dtype=jnp.int32)
    dest = jnp.arange(dp_size, dtype=jnp.int32)
    field = lane % 4
    value = jnp.where(
        field[None, :] == 0,
        starts[:, None],
        jnp.where(field[None, :] == 1, lengths[:, None], offsets[:, None]),
    )
    match = (owners[:, None, None] == dest[None, :, None]) & (
        rank[:, None, None] == (lane // 4)[None, None, :]
    )
    meta = jnp.sum(jnp.where(match, value[:, None, :], 0), axis=0)
    relative = lax.rem(owners - d + dp_size, dp_size)
    turn = dp_size // mp_size - 1 - relative // mp_size
    user_pos = lax.rem(relative, mp_size) * slots_pad + turn * per_pair + rank

    vmem = pl.BlockSpec(memory_space=pltpu.VMEM)
    smem = pl.BlockSpec(memory_space=pltpu.SMEM)
    anywhere = pl.BlockSpec(memory_space=pl.ANY)
    bf16, f32 = jnp.bfloat16, jnp.float32
    dma = pltpu.SemaphoreType.DMA
    arr, meta_in, state_in = pl.pallas_call(
        functools.partial(layer_kernel, dp_size, mp_size, per_pair),
        out_shape=(
            jax.ShapeDtypeStruct((pairs, WIN, quarter), bf16),
            jax.ShapeDtypeStruct((dp_size, 1, 128), jnp.int32),
            jax.ShapeDtypeStruct((mp_size, slots_pad, quarter), f32),
        ),
        in_specs=[smem, anywhere, vmem, vmem, vmem],
        out_specs=(anywhere, anywhere, anywhere),
        scratch_shapes=[
            pltpu.VMEM((rows // BLOCK + 1, BLOCK, D), bf16),
            pltpu.VMEM((mp_size, D, 4 * HEAD), bf16),
            pltpu.VMEM((D, D), bf16),
            pltpu.VMEM((slots, WIN, D), bf16),
            pltpu.VMEM((slots, 2, WIN, HEAD), f32),
            pltpu.VMEM((slots, 2, WIN, HEAD), bf16),
            pltpu.VMEM((slots, mp_size, WIN, quarter), bf16),
            pltpu.VMEM((mp_size, slots_pad, quarter), f32),
            dma,
            dma,
            dma((3,)),
            dma((3,)),
            dma((dp_size,)),
            dma((dp_size,)),
            dma((slots, mp_size)),
            dma((pairs,)),
            dma((mp_size,)),
            dma((mp_size,)),
        ],
        compiler_params=pltpu.CompilerParams(
            collective_id=0, has_side_effects=True, vmem_limit_bytes=60 * 1024 * 1024
        ),
        name="layer",
    )(meta, tokens.reshape(rows // BLOCK, BLOCK, D), w_uvqk, w_out, meta.reshape(dp_size, 1, 128))
    return pl.pallas_call(
        functools.partial(place_kernel, dp_size, per_pair),
        out_shape=(
            jax.ShapeDtypeStruct((rows, quarter), bf16),
            jax.ShapeDtypeStruct((user_count, quarter), bf16),
        ),
        in_specs=[smem, smem, vmem, vmem],
        out_specs=(vmem, vmem),
        scratch_shapes=[pltpu.VMEM((user_count, quarter), f32)],
        name="place",
    )(meta_in, user_pos, arr, state_in)


def solution(mesh):
    in_specs = (
        P("dp", None),
        P(None, "mp"),
        P(),
        P("dp", None),
        P("dp", None),
        P("dp", None),
        P("dp", None),
    )
    out_specs = (P("dp", "mp"), P("dp", "mp"))
    return jax.shard_map(
        per_device, mesh=mesh, in_specs=in_specs, out_specs=out_specs, check_vma=False
    )
```

```python
import functools

import jax
import jax.numpy as jnp
from jax import lax
from jax.experimental import pallas as pl
from jax.experimental.pallas import tpu as pltpu
from jax.sharding import PartitionSpec as P

D = 512
HEADS = 4
HEAD = D // HEADS
BLOCK = 128
MAXB = 2
WIN = MAXB * BLOCK
EPS = 1e-05
MESH = pl.DeviceIdType.MESH


def norm_rows(values):
    average = jnp.mean(values, axis=-1, keepdims=True)
    variance = jnp.mean(values * values, axis=-1, keepdims=True) - average * average
    return (values - average) * lax.rsqrt(variance + EPS)


def gather_kernel(
    dp_size, mp_size, per_pair,
    owner, hist_len, recv_offset, block_start, tok_hbm,
    table, user_pos, picked, row_sem,
):
    d = lax.axis_index("dp")
    m = lax.axis_index("mp")
    last_block = tok_hbm.shape[0] - 1
    slots = picked.shape[0]
    slots_pad = -(-per_pair // 8) * 8

    def clear(o, carry):
        for lane in range(4 * per_pair):
            table[o, 0, lane] = 0
        return carry

    lax.fori_loop(0, dp_size, clear, 0)

    def enter(u, carry):
        o = owner[0, u]
        rank = table[o, 0, 3]
        table[o, 0, 3] = rank + 1
        table[o, 0, 4 * rank] = block_start[0, u]
        table[o, 0, 4 * rank + 1] = hist_len[0, u]
        table[o, 0, 4 * rank + 2] = recv_offset[0, u]
        user_pos[u] = o * slots_pad + rank
        return carry

    lax.fori_loop(0, user_pos.shape[0], enter, 0)

    def copy(s, b):
        k = s // per_pair
        o = lax.rem(d + m + mp_size * k, dp_size)
        start = table[o, 0, 4 * (s - k * per_pair)]
        return pltpu.make_async_copy(
            tok_hbm.at[jnp.minimum(start + b, last_block)], picked.at[s, b], row_sem.at[s, b]
        )

    def begin(s, carry):
        for b in range(MAXB):
            copy(s, b).start()
        return carry

    def end(s, carry):
        for b in range(MAXB):
            copy(s, b).wait()
        return carry

    lax.fori_loop(0, slots, begin, 0)
    lax.fori_loop(0, slots, end, 0)


def layer_kernel(
    dp_size, mp_size, per_pair,
    rows_ref, w_ref, wout_ref, meta_ref,
    arr, meta_out, state_in,
    xin, wg, wop, send, state_out, meta_in,
    own_sem, w_send, w_recv, meta_send, meta_recv, row_send, row_recv, send_sem, recv_sem,
    state_send, state_recv, out_sem,
):
    d = lax.axis_index("dp")
    m = lax.axis_index("mp")
    quarter = D // mp_size
    reach = dp_size // mp_size
    slots = reach * per_pair

    own_copy = pltpu.make_async_copy(w_ref, wg.at[0], own_sem)
    own_copy.start()

    barrier = pltpu.get_barrier_semaphore()

    def greet(step, carry):
        o = lax.rem(d + step // mp_size, dp_size)
        q = lax.rem(m + lax.rem(step, mp_size), mp_size)
        pl.semaphore_signal(barrier, inc=1, device_id={"dp": o, "mp": q}, device_id_type=MESH)
        return carry

    lax.fori_loop(1, dp_size * mp_size, greet, 0)
    pl.semaphore_wait(barrier, dp_size * mp_size - 1)

    def flip(bits):
        if bits == 1:
            return m + 1 - 2 * lax.rem(m, 2)
        return lax.rem(m + 2, 4)

    def w_copy(src, slot, peer, index):
        return pltpu.make_async_remote_copy(
            src_ref=src, dst_ref=wg.at[slot], send_sem=w_send.at[index],
            recv_sem=w_recv.at[index], device_id={"mp": peer}, device_id_type=MESH,
        )

    far = w_copy(w_ref, 2, flip(2), 1)
    far.start()
    near = w_copy(w_ref, 1, flip(1), 0)
    near.start()
    relay = w_copy(wg.at[2], 3, flip(1), 2)

    def target(s):
        k = s // per_pair
        return lax.rem(d + m + mp_size * k, dp_size)

    def source(s):
        k = s // per_pair
        return lax.rem(d - m - mp_size * k + 2 * dp_size, dp_size), s - k * per_pair

    def row_copy(s):
        return pltpu.make_async_remote_copy(
            src_ref=rows_ref.at[s], dst_ref=xin.at[s], send_sem=row_send.at[s],
            recv_sem=row_recv.at[s], device_id={"dp": target(s)}, device_id_type=MESH,
        )

    def row_local(s):
        return pltpu.make_async_copy(rows_ref.at[s], xin.at[s], row_recv.at[s])

    def start_rows(s, carry):
        here = target(s) == d

        @pl.when(jnp.logical_not(here))
        def _():
            row_copy(s).start()

        @pl.when(here)
        def _():
            row_local(s).start()

        return carry

    def end_rows(s, carry):
        @pl.when(target(s) != d)
        def _():
            row_copy(s).wait_send()

        return carry

    lax.fori_loop(0, slots, start_rows, 0)

    def meta_copy(step):
        o = lax.rem(d + step, dp_size)
        return pltpu.make_async_remote_copy(
            src_ref=meta_ref.at[o], dst_ref=meta_in.at[d], send_sem=meta_send.at[step],
            recv_sem=meta_recv.at[d], device_id={"dp": o}, device_id_type=MESH,
        )

    def start_meta(step, carry):
        meta_copy(step).start()
        return carry

    lax.fori_loop(1, dp_size, start_meta, 0)
    pltpu.make_async_copy(meta_ref.at[d], meta_in.at[d], meta_recv.at[d]).start()

    for bits in range(mp_size):
        head = m
        if bits & 1:
            head = head + 1 - 2 * lax.rem(head, 2)
        if bits & 2:
            head = lax.rem(head + 2, 4)
        wop[bits * HEAD : (bits + 1) * HEAD, :] = wout_ref[
            pl.ds(pl.multiple_of(head * HEAD, HEAD), HEAD), :
        ]

    causal = lax.broadcasted_iota(jnp.int32, (BLOCK, BLOCK), 1) <= lax.broadcasted_iota(
        jnp.int32, (BLOCK, BLOCK), 0
    )
    half_scale = 0.5 * HEAD ** (-0.5)

    def scores(q, k):
        t = lax.dot_general(
            q, k, (((1,), (1,)), ((), ())), preferred_element_type=jnp.float32
        ) * half_scale
        return t + t * jnp.tanh(t)

    def one_head(rows_in, bits):
        h = jnp.dot(rows_in, wg[bits], preferred_element_type=jnp.float32) * 0.5
        p = (h + h * jnp.tanh(h)).astype(jnp.bfloat16)
        u, v, q, k = (p[:, i * HEAD : (i + 1) * HEAD] for i in range(4))
        low = jnp.where(causal, scores(q[:BLOCK], k[:BLOCK]), 0.0).astype(jnp.bfloat16)
        back = scores(q[BLOCK:], k[:BLOCK])
        diag = jnp.where(causal, scores(q[BLOCK:], k[BLOCK:]), 0.0)
        high = jnp.concatenate([back, diag], 1).astype(jnp.bfloat16)
        first = jnp.dot(low, v[:BLOCK], preferred_element_type=jnp.float32)
        second = jnp.dot(high, v, preferred_element_type=jnp.float32)
        return u, jnp.concatenate([first, second], 0) * (1.0 / WIN)

    def got_meta(src, carry):
        pltpu.make_async_copy(meta_ref.at[src], meta_in.at[src], meta_recv.at[src]).wait()
        return carry

    lax.fori_loop(0, dp_size, got_meta, 0)
    meta_back = pltpu.make_async_copy(meta_in, meta_out, out_sem)
    meta_back.start()

    own_copy.wait()
    near.wait()
    far.wait()
    relay.start()
    relay.wait()

    def send_copy(s, q):
        src, j = source(s)
        pair = src * per_pair + j
        return pltpu.make_async_remote_copy(
            src_ref=send.at[s, q], dst_ref=arr.at[pair], send_sem=send_sem.at[s, q],
            recv_sem=recv_sem.at[pair], device_id={"mp": q}, device_id_type=MESH,
        )

    picks = lax.broadcasted_iota(jnp.int32, (8, WIN), 1)
    lanes = lax.broadcasted_iota(jnp.int32, (1, 128), 1)

    def one_user(s, carry):
        row_local(s).wait()
        src, j = source(s)
        rows_in = xin[s].reshape(WIN, D).astype(jnp.float32)
        n = norm_rows(rows_in).astype(jnp.bfloat16)
        parts = [one_head(n, bits) for bits in range(mp_size)]
        a = jnp.concatenate([part[1] for part in parts], 1)
        g = jnp.concatenate([part[0] for part in parts], 1).astype(jnp.float32)
        gated = (norm_rows(a) * g).astype(jnp.bfloat16)
        y = jnp.dot(gated, wop[...], preferred_element_type=jnp.float32)
        y = (y + rows_in).astype(jnp.bfloat16)
        length = jnp.sum(
            jnp.where(lanes == 4 * j + 1, meta_in[src], 0), axis=1, keepdims=True
        )
        pick = jnp.where(picks == length - 1, 1.0, 0.0).astype(jnp.bfloat16)
        chosen = jnp.dot(pick, y, preferred_element_type=jnp.float32)
        for q in range(mp_size):
            send[s, q] = y[:, q * quarter : (q + 1) * quarter]
            state_out[s // per_pair, q, pl.ds(j, 1), :] = chosen[
                0:1, q * quarter : (q + 1) * quarter
            ]
        pair = src * per_pair + j
        for q in range(mp_size):

            @pl.when(m != q)
            def _():
                send_copy(s, q).start()

            @pl.when(m == q)
            def _():
                pltpu.make_async_copy(send.at[s, q], arr.at[pair], recv_sem.at[pair]).start()

        return carry

    lax.fori_loop(0, slots, one_user, 0)

    def state_step(step, first):
        k = step // mp_size
        q = step - k * mp_size
        src, _ = source(k * per_pair)
        own = jnp.logical_and(src == d, q == m)

        @pl.when(jnp.logical_not(own))
        def _():
            copy = pltpu.make_async_remote_copy(
                src_ref=state_out.at[k, q], dst_ref=state_in.at[d],
                send_sem=state_send.at[step], recv_sem=state_recv.at[d],
                device_id={"dp": src, "mp": q}, device_id_type=MESH,
            )
            if first:
                copy.start()
            else:
                copy.wait_send()

        if first:

            @pl.when(own)
            def _():
                pltpu.make_async_copy(
                    state_out.at[k, q], state_in.at[d], state_recv.at[d]
                ).start()

    def start_state(step, carry):
        state_step(step, True)
        return carry

    def end_state(step, carry):
        state_step(step, False)
        return carry

    lax.fori_loop(0, reach * mp_size, start_state, 0)
    meta_back.wait()

    def end_meta(step, carry):
        meta_copy(step).wait_send()
        return carry

    lax.fori_loop(1, dp_size, end_meta, 0)
    lax.fori_loop(0, slots, end_rows, 0)

    def sent(s, carry):
        for q in range(mp_size):

            @pl.when(m != q)
            def _():
                send_copy(s, q).wait_send()

        return carry

    lax.fori_loop(0, slots, sent, 0)
    lax.fori_loop(0, reach * mp_size, end_state, 0)

    def got(i, carry):
        pltpu.make_async_copy(send.at[0, 0], arr.at[i], recv_sem.at[i]).wait()
        return carry

    lax.fori_loop(0, dp_size * per_pair, got, 0)

    def got_state(o, carry):
        pltpu.make_async_copy(state_out.at[0, 0], state_in.at[o], state_recv.at[o]).wait()
        return carry

    lax.fori_loop(0, dp_size, got_state, 0)


def place_kernel(dp_size, per_pair, meta, user_pos, arr, state_in, packed, state, rows32):
    slots = state_in.shape[1]
    packed[...] = jnp.zeros(packed.shape, packed.dtype)
    row = lax.broadcasted_iota(jnp.int32, (BLOCK, packed.shape[1]), 0)

    def one(i, carry):
        src = i // per_pair
        j = i - src * per_pair
        length = meta[src, 0, 4 * j + 1]
        offset = meta[src, 0, 4 * j + 2]
        for b in range(MAXB):
            fill = length - b * BLOCK

            @pl.when(fill > 0)
            def _():
                value = arr[i, b * BLOCK : (b + 1) * BLOCK, :].astype(jnp.float32)
                value = jnp.where(row < fill, value, 0.0).astype(packed.dtype)
                packed[pl.ds(pl.multiple_of((offset + b) * BLOCK, BLOCK), BLOCK), :] = value

        return carry

    lax.fori_loop(0, dp_size * per_pair, one, 0)

    def pick(u, carry):
        pos = user_pos[u]
        q = pos // slots
        rows32[pl.ds(u, 1), :] = state_in[q, pl.ds(pos - q * slots, 1), :]
        return carry

    lax.fori_loop(0, state.shape[0], pick, 0)
    state[...] = rows32[...].astype(state.dtype)


def per_device(tokens, w_uvqk, w_out, hist_len, owner, recv_offset, block_start):
    dp_size = lax.axis_size("dp")
    mp_size = lax.axis_size("mp")
    user_count = hist_len.shape[1]
    per_pair = -(-user_count // dp_size)
    pairs = dp_size * per_pair
    reach = dp_size // mp_size
    slots = reach * per_pair
    slots_pad = -(-per_pair // 8) * 8
    quarter = D // mp_size
    rows = tokens.shape[0]

    vmem = pl.BlockSpec(memory_space=pltpu.VMEM)
    smem = pl.BlockSpec(memory_space=pltpu.SMEM)
    anywhere = pl.BlockSpec(memory_space=pl.ANY)
    bf16, f32 = jnp.bfloat16, jnp.float32
    dma = pltpu.SemaphoreType.DMA
    meta, user_pos, picked = pl.pallas_call(
        functools.partial(gather_kernel, dp_size, mp_size, per_pair),
        out_shape=(
            jax.ShapeDtypeStruct((dp_size, 1, 128), jnp.int32),
            jax.ShapeDtypeStruct((user_count,), jnp.int32),
            jax.ShapeDtypeStruct((slots, MAXB, BLOCK, D), bf16),
        ),
        in_specs=[smem, smem, smem, smem, anywhere],
        out_specs=(smem, smem, vmem),
        scratch_shapes=[dma((slots, MAXB))],
        name="gather",
    )(owner, hist_len, recv_offset, block_start, tokens.reshape(rows // BLOCK, BLOCK, D))
    arr, meta_in, state_in = pl.pallas_call(
        functools.partial(layer_kernel, dp_size, mp_size, per_pair),
        out_shape=(
            jax.ShapeDtypeStruct((pairs, WIN, quarter), bf16),
            jax.ShapeDtypeStruct((dp_size, 1, 128), jnp.int32),
            jax.ShapeDtypeStruct((dp_size, slots_pad, quarter), f32),
        ),
        in_specs=[anywhere, vmem, vmem, vmem],
        out_specs=(anywhere, anywhere, anywhere),
        scratch_shapes=[
            pltpu.VMEM((slots, MAXB, BLOCK, D), bf16),
            pltpu.VMEM((mp_size, D, 4 * HEAD), bf16),
            pltpu.VMEM((D, D), bf16),
            pltpu.VMEM((slots, mp_size, WIN, quarter), bf16),
            pltpu.VMEM((reach, mp_size, slots_pad, quarter), f32),
            pltpu.VMEM((dp_size, 1, 128), jnp.int32),
            dma,
            dma((3,)),
            dma((3,)),
            dma((dp_size,)),
            dma((dp_size,)),
            dma((slots,)),
            dma((slots,)),
            dma((slots, mp_size)),
            dma((pairs,)),
            dma((reach * mp_size,)),
            dma((dp_size,)),
            dma,
        ],
        compiler_params=pltpu.CompilerParams(
            collective_id=0, has_side_effects=True, vmem_limit_bytes=40 * 1024 * 1024
        ),
        name="layer",
    )(picked, w_uvqk, w_out, meta)
    return pl.pallas_call(
        functools.partial(place_kernel, dp_size, per_pair),
        out_shape=(
            jax.ShapeDtypeStruct((rows, quarter), bf16),
            jax.ShapeDtypeStruct((user_count, quarter), bf16),
        ),
        in_specs=[smem, smem, vmem, vmem],
        out_specs=(vmem, vmem),
        scratch_shapes=[pltpu.VMEM((user_count, quarter), f32)],
        name="place",
    )(meta_in, user_pos, arr, state_in)


def solution(mesh):
    in_specs = (
        P("dp", None),
        P(None, "mp"),
        P(),
        P("dp", None),
        P("dp", None),
        P("dp", None),
        P("dp", None),
    )
    out_specs = (P("dp", "mp"), P("dp", "mp"))
    return jax.shard_map(
        per_device, mesh=mesh, in_specs=in_specs, out_specs=out_specs, check_vma=False
    )
```

```python
import functools

import jax
import jax.numpy as jnp
from jax import lax
from jax.experimental import pallas as pl
from jax.experimental.pallas import tpu as pltpu
from jax.sharding import PartitionSpec as P

D = 512
HEADS = 4
HEAD = D // HEADS
BLOCK = 128
MAXB = 2
WIN = MAXB * BLOCK
EPS = 1e-05
MESH = pl.DeviceIdType.MESH


def norm_rows(values):
    average = jnp.mean(values, axis=-1, keepdims=True)
    variance = jnp.mean(values * values, axis=-1, keepdims=True) - average * average
    return (values - average) * lax.rsqrt(variance + EPS)


def gather_kernel(
    dp_size, mp_size, per_pair,
    owner, hist_len, recv_offset, block_start, tok_hbm,
    table, user_pos, picked, row_sem,
):
    d = lax.axis_index("dp")
    m = lax.axis_index("mp")
    last_block = tok_hbm.shape[0] - 1
    slots = picked.shape[0]

    def clear(o, carry):
        for lane in range(4 * per_pair):
            table[o, 0, lane] = 0
        return carry

    lax.fori_loop(0, dp_size, clear, 0)

    def enter(u, carry):
        o = owner[0, u]
        rank = table[o, 0, 3]
        table[o, 0, 3] = rank + 1
        table[o, 0, 4 * rank] = block_start[0, u]
        table[o, 0, 4 * rank + 1] = hist_len[0, u]
        table[o, 0, 4 * rank + 2] = recv_offset[0, u]
        user_pos[u] = o * per_pair + rank
        return carry

    lax.fori_loop(0, user_pos.shape[0], enter, 0)

    def copy(s, b):
        k = s // per_pair
        o = lax.rem(d + m + mp_size * k, dp_size)
        start = table[o, 0, 4 * (s - k * per_pair)]
        return pltpu.make_async_copy(
            tok_hbm.at[jnp.minimum(start + b, last_block)], picked.at[s, b], row_sem.at[s, b]
        )

    def begin(s, carry):
        for b in range(MAXB):
            copy(s, b).start()
        return carry

    def end(s, carry):
        for b in range(MAXB):
            copy(s, b).wait()
        return carry

    lax.fori_loop(0, slots, begin, 0)
    lax.fori_loop(0, slots, end, 0)


def layer_kernel(
    dp_size, mp_size, per_pair,
    rows_ref, w_ref, wout_ref, meta_ref,
    arr, meta_out, state_in,
    xin, wg, wop, send, state_out, meta_in,
    own_sem, w_send, w_recv, meta_send, meta_recv, row_send, row_recv, send_sem, recv_sem,
    state_send, state_recv, out_sem,
):
    d = lax.axis_index("dp")
    m = lax.axis_index("mp")
    quarter = D // mp_size
    reach = dp_size // mp_size
    slots = reach * per_pair

    own_copy = pltpu.make_async_copy(w_ref, wg.at[0], own_sem)
    own_copy.start()

    barrier = pltpu.get_barrier_semaphore()

    def greet(step, carry):
        o = lax.rem(d + step // mp_size, dp_size)
        q = lax.rem(m + lax.rem(step, mp_size), mp_size)
        pl.semaphore_signal(barrier, inc=1, device_id={"dp": o, "mp": q}, device_id_type=MESH)
        return carry

    lax.fori_loop(1, dp_size * mp_size, greet, 0)
    pl.semaphore_wait(barrier, dp_size * mp_size - 1)

    def flip(bits):
        if bits == 1:
            return m + 1 - 2 * lax.rem(m, 2)
        return lax.rem(m + 2, 4)

    def w_copy(src, slot, peer, index):
        return pltpu.make_async_remote_copy(
            src_ref=src, dst_ref=wg.at[slot], send_sem=w_send.at[index],
            recv_sem=w_recv.at[index], device_id={"mp": peer}, device_id_type=MESH,
        )

    far = w_copy(w_ref, 2, flip(2), 1)
    far.start()
    near = w_copy(w_ref, 1, flip(1), 0)
    near.start()
    relay = w_copy(wg.at[2], 3, flip(1), 2)

    def target(s):
        k = s // per_pair
        return lax.rem(d + m + mp_size * k, dp_size)

    def source(s):
        k = s // per_pair
        return lax.rem(d - m - mp_size * k + 2 * dp_size, dp_size), s - k * per_pair

    def row_copy(s):
        return pltpu.make_async_remote_copy(
            src_ref=rows_ref.at[s], dst_ref=xin.at[s], send_sem=row_send.at[s],
            recv_sem=row_recv.at[s], device_id={"dp": target(s)}, device_id_type=MESH,
        )

    def row_local(s):
        return pltpu.make_async_copy(rows_ref.at[s], xin.at[s], row_recv.at[s])

    def travels(s):
        k = s // per_pair
        return lax.rem(s - k * per_pair + k, 2) == 0

    def start_rows(s, carry):
        away = jnp.logical_and(travels(s), target(s) != d)

        @pl.when(away)
        def _():
            row_copy(s).start()

        @pl.when(jnp.logical_not(away))
        def _():
            row_local(s).start()

        return carry

    def end_rows(s, carry):
        @pl.when(jnp.logical_and(travels(s), target(s) != d))
        def _():
            row_copy(s).wait_send()

        return carry

    lax.fori_loop(0, slots, start_rows, 0)

    def meta_copy(step):
        o = lax.rem(d + step, dp_size)
        return pltpu.make_async_remote_copy(
            src_ref=meta_ref.at[o], dst_ref=meta_in.at[d], send_sem=meta_send.at[step],
            recv_sem=meta_recv.at[d], device_id={"dp": o}, device_id_type=MESH,
        )

    def start_meta(step, carry):
        meta_copy(step).start()
        return carry

    lax.fori_loop(1, dp_size, start_meta, 0)
    pltpu.make_async_copy(meta_ref.at[d], meta_in.at[d], meta_recv.at[d]).start()

    for bits in range(mp_size):
        head = m
        if bits & 1:
            head = head + 1 - 2 * lax.rem(head, 2)
        if bits & 2:
            head = lax.rem(head + 2, 4)
        wop[bits * HEAD : (bits + 1) * HEAD, :] = wout_ref[
            pl.ds(pl.multiple_of(head * HEAD, HEAD), HEAD), :
        ]

    causal = lax.broadcasted_iota(jnp.int32, (BLOCK, BLOCK), 1) <= lax.broadcasted_iota(
        jnp.int32, (BLOCK, BLOCK), 0
    )
    half_scale = 0.5 * HEAD ** (-0.5)

    def scores(q, k):
        t = lax.dot_general(
            q, k, (((1,), (1,)), ((), ())), preferred_element_type=jnp.float32
        ) * half_scale
        return t + t * jnp.tanh(t)

    def one_head(rows_in, bits):
        h = jnp.dot(rows_in, wg[bits], preferred_element_type=jnp.float32) * 0.5
        p = (h + h * jnp.tanh(h)).astype(jnp.bfloat16)
        u, v, q, k = (p[:, i * HEAD : (i + 1) * HEAD] for i in range(4))
        low = jnp.where(causal, scores(q[:BLOCK], k[:BLOCK]), 0.0).astype(jnp.bfloat16)
        back = scores(q[BLOCK:], k[:BLOCK])
        diag = jnp.where(causal, scores(q[BLOCK:], k[BLOCK:]), 0.0)
        high = jnp.concatenate([back, diag], 1).astype(jnp.bfloat16)
        first = jnp.dot(low, v[:BLOCK], preferred_element_type=jnp.float32)
        second = jnp.dot(high, v, preferred_element_type=jnp.float32)
        return u, jnp.concatenate([first, second], 0) * (1.0 / WIN)

    def got_meta(src, carry):
        pltpu.make_async_copy(meta_ref.at[src], meta_in.at[src], meta_recv.at[src]).wait()
        return carry

    lax.fori_loop(0, dp_size, got_meta, 0)
    meta_back = pltpu.make_async_copy(meta_in, meta_out, out_sem)
    meta_back.start()

    own_copy.wait()
    near.wait()
    far.wait()
    relay.start()
    relay.wait()

    def route(s):
        src, j = source(s)
        moved = travels(s)
        home = jnp.where(moved, src, d)
        there = jnp.where(moved, d, target(s))
        return moved, home, there, j

    def send_copy(s, q):
        _, home, there, j = route(s)
        pair = home * per_pair + j
        return pltpu.make_async_remote_copy(
            src_ref=send.at[s, q], dst_ref=arr.at[pair], send_sem=send_sem.at[s, q],
            recv_sem=recv_sem.at[pair], device_id={"dp": there, "mp": q}, device_id_type=MESH,
        )

    def state_copy(s, q):
        _, home, there, j = route(s)
        pair = there * per_pair + j
        return pltpu.make_async_remote_copy(
            src_ref=state_out.at[s, q], dst_ref=state_in.at[pair], send_sem=state_send.at[s, q],
            recv_sem=state_recv.at[pair], device_id={"dp": home, "mp": q}, device_id_type=MESH,
        )

    picks = lax.broadcasted_iota(jnp.int32, (8, WIN), 1)
    lanes = lax.broadcasted_iota(jnp.int32, (1, 128), 1)
    positions = lax.broadcasted_iota(jnp.int32, (WIN, D), 0)

    def one_user(s):
        row_local(s).wait()
        moved, home, there, j = route(s)
        src, _ = source(s)
        rows_in = xin[s].reshape(WIN, D).astype(jnp.float32)
        n = norm_rows(rows_in).astype(jnp.bfloat16)
        parts = [one_head(n, bits) for bits in range(mp_size)]
        a = jnp.concatenate([part[1] for part in parts], 1)
        g = jnp.concatenate([part[0] for part in parts], 1).astype(jnp.float32)
        gated = (norm_rows(a) * g).astype(jnp.bfloat16)
        y = jnp.dot(gated, wop[...], preferred_element_type=jnp.float32)
        entry = jnp.where(moved, meta_in[src], meta_ref[target(s)])
        length = jnp.sum(jnp.where(lanes == 4 * j + 1, entry, 0), axis=1, keepdims=True)
        y = jnp.where(positions < length, y + rows_in, 0.0).astype(jnp.bfloat16)
        for q in range(mp_size):
            send[s, q] = y[:, q * quarter : (q + 1) * quarter]
        pick = jnp.where(picks == length - 1, 1.0, 0.0).astype(jnp.bfloat16)
        chosen = jnp.dot(pick, y, preferred_element_type=jnp.float32)
        for q in range(mp_size):
            state_out[s, q] = chosen[:, q * quarter : (q + 1) * quarter]
        pair = home * per_pair + j
        state_pair = there * per_pair + j
        for q in range(mp_size):
            own = jnp.logical_and(there == d, q == m)

            @pl.when(jnp.logical_not(own))
            def _():
                send_copy(s, q).start()

            @pl.when(own)
            def _():
                pltpu.make_async_copy(send.at[s, q], arr.at[pair], recv_sem.at[pair]).start()

        for q in range(mp_size):
            own = jnp.logical_and(home == d, q == m)

            @pl.when(jnp.logical_not(own))
            def _():
                state_copy(s, q).start()

            @pl.when(own)
            def _():
                pltpu.make_async_copy(
                    state_out.at[s, q], state_in.at[state_pair], state_recv.at[state_pair]
                ).start()

    def turn(i, carry):
        late = i // slots
        s = i - late * slots

        @pl.when(travels(s) == (late == 1))
        def _():
            one_user(s)

        return carry

    lax.fori_loop(0, 2 * slots, turn, 0)
    meta_back.wait()

    def end_meta(step, carry):
        meta_copy(step).wait_send()
        return carry

    lax.fori_loop(1, dp_size, end_meta, 0)
    lax.fori_loop(0, slots, end_rows, 0)

    def sent(s, carry):
        _, home, there, _ = route(s)
        for q in range(mp_size):

            @pl.when(jnp.logical_not(jnp.logical_and(there == d, q == m)))
            def _():
                send_copy(s, q).wait_send()

            @pl.when(jnp.logical_not(jnp.logical_and(home == d, q == m)))
            def _():
                state_copy(s, q).wait_send()

        return carry

    lax.fori_loop(0, slots, sent, 0)

    def got(i, carry):
        pltpu.make_async_copy(send.at[0, 0], arr.at[i], recv_sem.at[i]).wait()
        pltpu.make_async_copy(state_out.at[0, 0], state_in.at[i], state_recv.at[i]).wait()
        return carry

    lax.fori_loop(0, dp_size * per_pair, got, 0)


def place_kernel(
    dp_size, per_pair,
    meta, user_pos, arr, state_in,
    packed, state,
    held, zero, rows32, used, in_sem, out_sem,
):
    pairs = dp_size * per_pair
    blocks = packed.shape[0]

    def bring(i):
        return pltpu.make_async_copy(arr.at[i], held.at[i], in_sem.at[i])

    def put(source, block):
        return pltpu.make_async_copy(source, packed.at[block], out_sem.at[block])

    def begin(i, carry):
        bring(i).start()
        return carry

    lax.fori_loop(0, pairs, begin, 0)
    zero[...] = jnp.zeros(zero.shape, zero.dtype)
    for block in range(blocks):
        used[block] = 0

    def pick(u, carry):
        rows32[pl.ds(u, 1), :] = state_in[user_pos[u], 0:1, :]
        return carry

    lax.fori_loop(0, state.shape[0], pick, 0)
    state[...] = rows32[...].astype(state.dtype)

    def one(i, carry):
        src = i // per_pair
        j = i - src * per_pair
        length = meta[src, 0, 4 * j + 1]
        offset = meta[src, 0, 4 * j + 2]
        bring(i).wait()
        for b in range(MAXB):

            @pl.when(length > b * BLOCK)
            def _():
                used[offset + b] = 1
                put(held.at[i, pl.ds(b * BLOCK, BLOCK)], offset + b).start()

        return carry

    lax.fori_loop(0, pairs, one, 0)

    def fill(block, carry):
        @pl.when(used[block] == 0)
        def _():
            put(zero, block).start()

        return carry

    lax.fori_loop(0, blocks, fill, 0)

    def end(block, carry):
        put(zero, block).wait()
        return carry

    lax.fori_loop(0, blocks, end, 0)


def per_device(tokens, w_uvqk, w_out, hist_len, owner, recv_offset, block_start):
    dp_size = lax.axis_size("dp")
    mp_size = lax.axis_size("mp")
    user_count = hist_len.shape[1]
    per_pair = -(-user_count // dp_size)
    pairs = dp_size * per_pair
    reach = dp_size // mp_size
    slots = reach * per_pair
    quarter = D // mp_size
    rows = tokens.shape[0]

    vmem = pl.BlockSpec(memory_space=pltpu.VMEM)
    smem = pl.BlockSpec(memory_space=pltpu.SMEM)
    anywhere = pl.BlockSpec(memory_space=pl.ANY)
    bf16, f32 = jnp.bfloat16, jnp.float32
    dma = pltpu.SemaphoreType.DMA
    meta, user_pos, picked = pl.pallas_call(
        functools.partial(gather_kernel, dp_size, mp_size, per_pair),
        out_shape=(
            jax.ShapeDtypeStruct((dp_size, 1, 128), jnp.int32),
            jax.ShapeDtypeStruct((user_count,), jnp.int32),
            jax.ShapeDtypeStruct((slots, MAXB, BLOCK, D), bf16),
        ),
        in_specs=[smem, smem, smem, smem, anywhere],
        out_specs=(smem, smem, vmem),
        scratch_shapes=[dma((slots, MAXB))],
        name="gather",
    )(owner, hist_len, recv_offset, block_start, tokens.reshape(rows // BLOCK, BLOCK, D))
    arr, meta_in, state_in = pl.pallas_call(
        functools.partial(layer_kernel, dp_size, mp_size, per_pair),
        out_shape=(
            jax.ShapeDtypeStruct((pairs, WIN, quarter), bf16),
            jax.ShapeDtypeStruct((dp_size, 1, 128), jnp.int32),
            jax.ShapeDtypeStruct((pairs, 8, quarter), f32),
        ),
        in_specs=[anywhere, vmem, vmem, vmem],
        out_specs=(anywhere, anywhere, anywhere),
        scratch_shapes=[
            pltpu.VMEM((slots, MAXB, BLOCK, D), bf16),
            pltpu.VMEM((mp_size, D, 4 * HEAD), bf16),
            pltpu.VMEM((D, D), bf16),
            pltpu.VMEM((slots, mp_size, WIN, quarter), bf16),
            pltpu.VMEM((slots, mp_size, 8, quarter), f32),
            pltpu.VMEM((dp_size, 1, 128), jnp.int32),
            dma,
            dma((3,)),
            dma((3,)),
            dma((dp_size,)),
            dma((dp_size,)),
            dma((slots,)),
            dma((slots,)),
            dma((slots, mp_size)),
            dma((pairs,)),
            dma((slots, mp_size)),
            dma((pairs,)),
            dma,
        ],
        compiler_params=pltpu.CompilerParams(
            collective_id=0, has_side_effects=True, vmem_limit_bytes=60 * 1024 * 1024
        ),
        name="layer",
    )(picked, w_uvqk, w_out, meta)
    packed, state = pl.pallas_call(
        functools.partial(place_kernel, dp_size, per_pair),
        out_shape=(
            jax.ShapeDtypeStruct((rows // BLOCK, BLOCK, quarter), bf16),
            jax.ShapeDtypeStruct((user_count, quarter), bf16),
        ),
        in_specs=[smem, smem, anywhere, vmem],
        out_specs=(anywhere, vmem),
        scratch_shapes=[
            pltpu.VMEM((pairs, WIN, quarter), bf16),
            pltpu.VMEM((BLOCK, quarter), bf16),
            pltpu.VMEM((user_count, quarter), f32),
            pltpu.SMEM((rows // BLOCK,), jnp.int32),
            dma((pairs,)),
            dma((rows // BLOCK,)),
        ],
        compiler_params=pltpu.CompilerParams(vmem_limit_bytes=60 * 1024 * 1024),
        name="place",
    )(meta_in, user_pos, arr, state_in)
    return packed.reshape(rows, quarter), state


def solution(mesh):
    in_specs = (
        P("dp", None),
        P(None, "mp"),
        P(),
        P("dp", None),
        P("dp", None),
        P("dp", None),
        P("dp", None),
    )
    out_specs = (P("dp", "mp"), P("dp", "mp"))
    return jax.shard_map(
        per_device, mesh=mesh, in_specs=in_specs, out_specs=out_specs, check_vma=False
    )
```

```python
import functools

import jax
import jax.numpy as jnp
from jax import lax
from jax.experimental import pallas as pl
from jax.experimental.pallas import tpu as pltpu
from jax.sharding import PartitionSpec as P

D = 512
HEADS = 4
HEAD = D // HEADS
BLOCK = 128
MAXB = 2
WIN = MAXB * BLOCK
EPS = 1e-05
MESH = pl.DeviceIdType.MESH


def norm_rows(values):
    average = jnp.mean(values, axis=-1, keepdims=True)
    variance = jnp.mean(values * values, axis=-1, keepdims=True) - average * average
    return (values - average) * lax.rsqrt(variance + EPS)


def gather_kernel(
    dp_size, mp_size, per_pair,
    owner, hist_len, recv_offset, block_start, tok_hbm,
    table, user_pos, picked, row_sem,
):
    d = lax.axis_index("dp")
    m = lax.axis_index("mp")
    last_block = tok_hbm.shape[0] - 1
    slots = picked.shape[0]

    def clear(o, carry):
        for lane in range(4 * per_pair):
            table[o, 0, lane] = 0
        return carry

    lax.fori_loop(0, dp_size, clear, 0)

    def enter(u, carry):
        o = owner[0, u]
        rank = table[o, 0, 3]
        table[o, 0, 3] = rank + 1
        table[o, 0, 4 * rank] = block_start[0, u]
        table[o, 0, 4 * rank + 1] = hist_len[0, u]
        table[o, 0, 4 * rank + 2] = recv_offset[0, u]
        user_pos[u] = o * per_pair + rank
        return carry

    lax.fori_loop(0, user_pos.shape[0], enter, 0)

    def copy(s, b):
        k = s // per_pair
        o = lax.rem(d + m + mp_size * k, dp_size)
        start = table[o, 0, 4 * (s - k * per_pair)]
        return pltpu.make_async_copy(
            tok_hbm.at[jnp.minimum(start + b, last_block)], picked.at[s, b], row_sem.at[s, b]
        )

    def begin(s, carry):
        for b in range(MAXB):
            copy(s, b).start()
        return carry

    def end(s, carry):
        for b in range(MAXB):
            copy(s, b).wait()
        return carry

    lax.fori_loop(0, slots, begin, 0)
    lax.fori_loop(0, slots, end, 0)


def layer_kernel(
    dp_size, mp_size, per_pair,
    rows_ref, w_ref, wout_ref, meta_ref,
    arr, meta_out, state_in,
    xin, wg, wop, send, state_out, meta_in,
    own_sem, w_send, w_recv, meta_send, meta_recv, row_send, row_recv, send_sem, recv_sem,
    state_send, state_recv, out_sem,
):
    d = lax.axis_index("dp")
    m = lax.axis_index("mp")
    quarter = D // mp_size
    reach = dp_size // mp_size
    slots = reach * per_pair

    own_copy = pltpu.make_async_copy(w_ref, wg.at[0], own_sem)
    own_copy.start()

    barrier = pltpu.get_barrier_semaphore()

    def greet(step, carry):
        o = lax.rem(d + step // mp_size, dp_size)
        q = lax.rem(m + lax.rem(step, mp_size), mp_size)
        pl.semaphore_signal(barrier, inc=1, device_id={"dp": o, "mp": q}, device_id_type=MESH)
        return carry

    lax.fori_loop(1, dp_size * mp_size, greet, 0)
    pl.semaphore_wait(barrier, dp_size * mp_size - 1)

    def flip(bits):
        if bits == 1:
            return m + 1 - 2 * lax.rem(m, 2)
        return lax.rem(m + 2, 4)

    def w_copy(src, slot, peer, index):
        return pltpu.make_async_remote_copy(
            src_ref=src, dst_ref=wg.at[slot], send_sem=w_send.at[index],
            recv_sem=w_recv.at[index], device_id={"mp": peer}, device_id_type=MESH,
        )

    far = w_copy(w_ref, 2, flip(2), 1)
    far.start()
    near = w_copy(w_ref, 1, flip(1), 0)
    near.start()
    relay = w_copy(wg.at[2], 3, flip(1), 2)

    def target(s):
        k = s // per_pair
        return lax.rem(d + m + mp_size * k, dp_size)

    def source(s):
        k = s // per_pair
        return lax.rem(d - m - mp_size * k + 2 * dp_size, dp_size), s - k * per_pair

    def row_copy(s):
        return pltpu.make_async_remote_copy(
            src_ref=rows_ref.at[s], dst_ref=xin.at[s], send_sem=row_send.at[s],
            recv_sem=row_recv.at[s], device_id={"dp": target(s)}, device_id_type=MESH,
        )

    def row_local(s):
        return pltpu.make_async_copy(rows_ref.at[s], xin.at[s], row_recv.at[s])

    def travels(s):
        k = s // per_pair
        return s - k * per_pair == 0

    def start_rows(s, carry):
        away = jnp.logical_and(travels(s), target(s) != d)

        @pl.when(away)
        def _():
            row_copy(s).start()

        @pl.when(jnp.logical_not(away))
        def _():
            row_local(s).start()

        return carry

    def end_rows(s, carry):
        @pl.when(jnp.logical_and(travels(s), target(s) != d))
        def _():
            row_copy(s).wait_send()

        return carry

    lax.fori_loop(0, slots, start_rows, 0)

    def meta_copy(step):
        o = lax.rem(d + step, dp_size)
        return pltpu.make_async_remote_copy(
            src_ref=meta_ref.at[o], dst_ref=meta_in.at[d], send_sem=meta_send.at[step],
            recv_sem=meta_recv.at[d], device_id={"dp": o}, device_id_type=MESH,
        )

    def start_meta(step, carry):
        meta_copy(step).start()
        return carry

    lax.fori_loop(1, dp_size, start_meta, 0)
    pltpu.make_async_copy(meta_ref.at[d], meta_in.at[d], meta_recv.at[d]).start()

    for bits in range(mp_size):
        head = m
        if bits & 1:
            head = head + 1 - 2 * lax.rem(head, 2)
        if bits & 2:
            head = lax.rem(head + 2, 4)
        wop[bits * HEAD : (bits + 1) * HEAD, :] = wout_ref[
            pl.ds(pl.multiple_of(head * HEAD, HEAD), HEAD), :
        ]

    causal = lax.broadcasted_iota(jnp.int32, (BLOCK, BLOCK), 1) <= lax.broadcasted_iota(
        jnp.int32, (BLOCK, BLOCK), 0
    )
    half_scale = 0.5 * HEAD ** (-0.5)

    def scores(q, k):
        t = lax.dot_general(
            q, k, (((1,), (1,)), ((), ())), preferred_element_type=jnp.float32
        ) * half_scale
        return t + t * jnp.tanh(t)

    def one_head(rows_in, bits):
        h = jnp.dot(rows_in, wg[bits], preferred_element_type=jnp.float32) * 0.5
        p = (h + h * jnp.tanh(h)).astype(jnp.bfloat16)
        u, v, q, k = (p[:, i * HEAD : (i + 1) * HEAD] for i in range(4))
        low = jnp.where(causal, scores(q[:BLOCK], k[:BLOCK]), 0.0).astype(jnp.bfloat16)
        back = scores(q[BLOCK:], k[:BLOCK])
        diag = jnp.where(causal, scores(q[BLOCK:], k[BLOCK:]), 0.0)
        high = jnp.concatenate([back, diag], 1).astype(jnp.bfloat16)
        first = jnp.dot(low, v[:BLOCK], preferred_element_type=jnp.float32)
        second = jnp.dot(high, v, preferred_element_type=jnp.float32)
        return u, jnp.concatenate([first, second], 0) * (1.0 / WIN)

    def got_meta(src, carry):
        pltpu.make_async_copy(meta_ref.at[src], meta_in.at[src], meta_recv.at[src]).wait()
        return carry

    lax.fori_loop(0, dp_size, got_meta, 0)
    meta_back = pltpu.make_async_copy(meta_in, meta_out, out_sem)
    meta_back.start()

    own_copy.wait()
    near.wait()
    far.wait()
    relay.start()
    relay.wait()

    def route(s):
        src, j = source(s)
        moved = travels(s)
        home = jnp.where(moved, src, d)
        there = jnp.where(moved, d, target(s))
        return moved, home, there, j

    def send_copy(s, q):
        _, home, there, j = route(s)
        pair = home * per_pair + j
        return pltpu.make_async_remote_copy(
            src_ref=send.at[s, q], dst_ref=arr.at[pair], send_sem=send_sem.at[s, q],
            recv_sem=recv_sem.at[pair], device_id={"dp": there, "mp": q}, device_id_type=MESH,
        )

    def state_copy(s, q):
        _, home, there, j = route(s)
        pair = there * per_pair + j
        return pltpu.make_async_remote_copy(
            src_ref=state_out.at[s, q], dst_ref=state_in.at[pair], send_sem=state_send.at[s, q],
            recv_sem=state_recv.at[pair], device_id={"dp": home, "mp": q}, device_id_type=MESH,
        )

    picks = lax.broadcasted_iota(jnp.int32, (8, WIN), 1)
    lanes = lax.broadcasted_iota(jnp.int32, (1, 128), 1)
    positions = lax.broadcasted_iota(jnp.int32, (WIN, D), 0)

    def one_user(s):
        row_local(s).wait()
        moved, home, there, j = route(s)
        src, _ = source(s)
        rows_in = xin[s].reshape(WIN, D).astype(jnp.float32)
        n = norm_rows(rows_in).astype(jnp.bfloat16)
        parts = [one_head(n, bits) for bits in range(mp_size)]
        a = jnp.concatenate([part[1] for part in parts], 1)
        g = jnp.concatenate([part[0] for part in parts], 1).astype(jnp.float32)
        gated = (norm_rows(a) * g).astype(jnp.bfloat16)
        y = jnp.dot(gated, wop[...], preferred_element_type=jnp.float32)
        entry = jnp.where(moved, meta_in[src], meta_ref[target(s)])
        length = jnp.sum(jnp.where(lanes == 4 * j + 1, entry, 0), axis=1, keepdims=True)
        y = jnp.where(positions < length, y + rows_in, 0.0).astype(jnp.bfloat16)
        for q in range(mp_size):
            send[s, q] = y[:, q * quarter : (q + 1) * quarter]
        pick = jnp.where(picks == length - 1, 1.0, 0.0).astype(jnp.bfloat16)
        chosen = jnp.dot(pick, y, preferred_element_type=jnp.float32)
        for q in range(mp_size):
            state_out[s, q] = chosen[:, q * quarter : (q + 1) * quarter]
        pair = home * per_pair + j
        state_pair = there * per_pair + j
        for q in range(mp_size):
            own = jnp.logical_and(there == d, q == m)

            @pl.when(jnp.logical_not(own))
            def _():
                send_copy(s, q).start()

            @pl.when(own)
            def _():
                pltpu.make_async_copy(send.at[s, q], arr.at[pair], recv_sem.at[pair]).start()

        for q in range(mp_size):
            own = jnp.logical_and(home == d, q == m)

            @pl.when(jnp.logical_not(own))
            def _():
                state_copy(s, q).start()

            @pl.when(own)
            def _():
                pltpu.make_async_copy(
                    state_out.at[s, q], state_in.at[state_pair], state_recv.at[state_pair]
                ).start()

    def turn(i, carry):
        late = i // slots
        s = i - late * slots
        s = jnp.where(late == 0, slots - 1 - s, s)

        @pl.when(travels(s) == (late == 1))
        def _():
            one_user(s)

        return carry

    lax.fori_loop(0, 2 * slots, turn, 0)
    meta_back.wait()

    def end_meta(step, carry):
        meta_copy(step).wait_send()
        return carry

    lax.fori_loop(1, dp_size, end_meta, 0)
    lax.fori_loop(0, slots, end_rows, 0)

    def sent(s, carry):
        _, home, there, _ = route(s)
        for q in range(mp_size):

            @pl.when(jnp.logical_not(jnp.logical_and(there == d, q == m)))
            def _():
                send_copy(s, q).wait_send()

            @pl.when(jnp.logical_not(jnp.logical_and(home == d, q == m)))
            def _():
                state_copy(s, q).wait_send()

        return carry

    lax.fori_loop(0, slots, sent, 0)

    def got(i, carry):
        pltpu.make_async_copy(send.at[0, 0], arr.at[i], recv_sem.at[i]).wait()
        pltpu.make_async_copy(state_out.at[0, 0], state_in.at[i], state_recv.at[i]).wait()
        return carry

    lax.fori_loop(0, dp_size * per_pair, got, 0)


def place_kernel(
    dp_size, per_pair,
    meta, user_pos, arr, state_in,
    packed, state,
    held, zero, rows32, used, in_sem, out_sem,
):
    pairs = dp_size * per_pair
    blocks = packed.shape[0]

    def bring(i):
        return pltpu.make_async_copy(arr.at[i], held.at[i], in_sem.at[i])

    def put(source, block):
        return pltpu.make_async_copy(source, packed.at[block], out_sem.at[block])

    def begin(i, carry):
        bring(i).start()
        return carry

    lax.fori_loop(0, pairs, begin, 0)
    zero[...] = jnp.zeros(zero.shape, zero.dtype)
    for block in range(blocks):
        used[block] = 0

    def pick(u, carry):
        rows32[pl.ds(u, 1), :] = state_in[user_pos[u], 0:1, :]
        return carry

    lax.fori_loop(0, state.shape[0], pick, 0)
    state[...] = rows32[...].astype(state.dtype)

    def one(i, carry):
        src = i // per_pair
        j = i - src * per_pair
        length = meta[src, 0, 4 * j + 1]
        offset = meta[src, 0, 4 * j + 2]
        bring(i).wait()
        for b in range(MAXB):

            @pl.when(length > b * BLOCK)
            def _():
                used[offset + b] = 1
                put(held.at[i, pl.ds(b * BLOCK, BLOCK)], offset + b).start()

        return carry

    lax.fori_loop(0, pairs, one, 0)

    def fill(block, carry):
        @pl.when(used[block] == 0)
        def _():
            put(zero, block).start()

        return carry

    lax.fori_loop(0, blocks, fill, 0)

    def end(block, carry):
        put(zero, block).wait()
        return carry

    lax.fori_loop(0, blocks, end, 0)


def per_device(tokens, w_uvqk, w_out, hist_len, owner, recv_offset, block_start):
    dp_size = lax.axis_size("dp")
    mp_size = lax.axis_size("mp")
    user_count = hist_len.shape[1]
    per_pair = -(-user_count // dp_size)
    pairs = dp_size * per_pair
    reach = dp_size // mp_size
    slots = reach * per_pair
    quarter = D // mp_size
    rows = tokens.shape[0]

    vmem = pl.BlockSpec(memory_space=pltpu.VMEM)
    smem = pl.BlockSpec(memory_space=pltpu.SMEM)
    anywhere = pl.BlockSpec(memory_space=pl.ANY)
    bf16, f32 = jnp.bfloat16, jnp.float32
    dma = pltpu.SemaphoreType.DMA
    meta, user_pos, picked = pl.pallas_call(
        functools.partial(gather_kernel, dp_size, mp_size, per_pair),
        out_shape=(
            jax.ShapeDtypeStruct((dp_size, 1, 128), jnp.int32),
            jax.ShapeDtypeStruct((user_count,), jnp.int32),
            jax.ShapeDtypeStruct((slots, MAXB, BLOCK, D), bf16),
        ),
        in_specs=[smem, smem, smem, smem, anywhere],
        out_specs=(smem, smem, vmem),
        scratch_shapes=[dma((slots, MAXB))],
        name="gather",
    )(owner, hist_len, recv_offset, block_start, tokens.reshape(rows // BLOCK, BLOCK, D))
    arr, meta_in, state_in = pl.pallas_call(
        functools.partial(layer_kernel, dp_size, mp_size, per_pair),
        out_shape=(
            jax.ShapeDtypeStruct((pairs, WIN, quarter), bf16),
            jax.ShapeDtypeStruct((dp_size, 1, 128), jnp.int32),
            jax.ShapeDtypeStruct((pairs, 8, quarter), f32),
        ),
        in_specs=[anywhere, vmem, vmem, vmem],
        out_specs=(anywhere, anywhere, anywhere),
        scratch_shapes=[
            pltpu.VMEM((slots, MAXB, BLOCK, D), bf16),
            pltpu.VMEM((mp_size, D, 4 * HEAD), bf16),
            pltpu.VMEM((D, D), bf16),
            pltpu.VMEM((slots, mp_size, WIN, quarter), bf16),
            pltpu.VMEM((slots, mp_size, 8, quarter), f32),
            pltpu.VMEM((dp_size, 1, 128), jnp.int32),
            dma,
            dma((3,)),
            dma((3,)),
            dma((dp_size,)),
            dma((dp_size,)),
            dma((slots,)),
            dma((slots,)),
            dma((slots, mp_size)),
            dma((pairs,)),
            dma((slots, mp_size)),
            dma((pairs,)),
            dma,
        ],
        compiler_params=pltpu.CompilerParams(
            collective_id=0, has_side_effects=True, vmem_limit_bytes=60 * 1024 * 1024
        ),
        name="layer",
    )(picked, w_uvqk, w_out, meta)
    packed, state = pl.pallas_call(
        functools.partial(place_kernel, dp_size, per_pair),
        out_shape=(
            jax.ShapeDtypeStruct((rows // BLOCK, BLOCK, quarter), bf16),
            jax.ShapeDtypeStruct((user_count, quarter), bf16),
        ),
        in_specs=[smem, smem, anywhere, vmem],
        out_specs=(anywhere, vmem),
        scratch_shapes=[
            pltpu.VMEM((pairs, WIN, quarter), bf16),
            pltpu.VMEM((BLOCK, quarter), bf16),
            pltpu.VMEM((user_count, quarter), f32),
            pltpu.SMEM((rows // BLOCK,), jnp.int32),
            dma((pairs,)),
            dma((rows // BLOCK,)),
        ],
        compiler_params=pltpu.CompilerParams(vmem_limit_bytes=60 * 1024 * 1024),
        name="place",
    )(meta_in, user_pos, arr, state_in)
    return packed.reshape(rows, quarter), state


def solution(mesh):
    in_specs = (
        P("dp", None),
        P(None, "mp"),
        P(),
        P("dp", None),
        P("dp", None),
        P("dp", None),
        P("dp", None),
    )
    out_specs = (P("dp", "mp"), P("dp", "mp"))
    return jax.shard_map(
        per_device, mesh=mesh, in_specs=in_specs, out_specs=out_specs, check_vma=False
    )
```
